32 devices in a mesh: groups: 1, ep: 16 (over z, y, x), role: 2 (over core).
Axes of the slice: x: 2, y: 2, z: 4, core: 2. Of those that a mesh axis runs over, the one named last changes fastest.
Arguments:
- residual: bfloat16 [192, 2880], P(('groups', 'ep', 'role')), may hold values from -1.796875 to 1.796875
- queries: bfloat16 [192, 2880], P(('groups', 'ep', 'role')), may hold values from -150 to 150
- key_new: bfloat16 [192, 320], P(('groups', 'ep', 'role')), may hold values from -6 to 6
- value_new: bfloat16 [192, 320], P(('groups', 'ep', 'role')), may hold values from -6 to 6
- key_cache: bfloat16 [192, 128, 320], P(('groups', 'ep', 'role')), may hold values from -6 to 6
- value_cache: bfloat16 [192, 128, 320], P(('groups', 'ep', 'role')), may hold values from -6 to 6
- lengths: int32 [192], P(('groups', 'ep', 'role')), may hold values from 1 to 512
- sink_logits: float32 [45], replicated, may hold values from -6 to 6
- norm_gain: float32 [2880], replicated, may hold values from 0.1 to 1.9
- route_ids: int32 [192, 4], P(('groups', 'ep')), may hold values from 0 to 7, all different within a row; in each aligned block of 12 rows (0 to 11, 12 to 23, ...) at most 6 rows name the same one
- route_logits: float32 [192, 4], P(('groups', 'ep')), may hold values from -1 to 1
- up_weight: bfloat16 [2880, 11520], P(None, ('ep', 'role')), may hold values from -0.109375 to 0.109375
- down_weight: bfloat16 [11520, 2880], P(('ep', 'role')), may hold values from -0.15625 to 0.15625
Outputs:
- layer_out: bfloat16 [192, 2880], P(('groups', 'ep', 'role'))
The draws below stay inside these ranges and needn't reach their ends.
Inputs may be any that keep to these rules, and one draw needn't show every extreme that they name: `route_ids`: in each aligned block of 12 rows (the tokens of one index of ep) no expert is named more than 6 times, a bound that some block reaches.
All inputs are finite; a program needn't handle non-finite values.
Results may differ from the reference program's by a relative error of at most 0.0095.
Values may be sent and summed in bfloat16 or wider, within the bound.
A program may use at most 64 MiB of HBM per device.

```python
import math
import jax
import jax.numpy as jnp
import numpy as np
from jax import lax

D = 2880
HD = 64
QH = 45
KVH = 5
WIN = 128
TOPK = 4
HID_DEV = 360
TOK_DEV = 6
CAP = 6
EXPERTS = 8
FF = 1440
TOKENS = 192
N_EP = 16
N_ROLE = 2


def draw_queries(key, part):
    base = jax.random.normal(jax.random.fold_in(key, 11), (TOKENS, QH * HD), jnp.float32)
    return jnp.clip(base, -6.0, 6.0).astype(jnp.bfloat16)


def with_ends(array, key, least, high):
    index_at = [jax.random.randint(jax.random.fold_in(key, axis), (), 0, length) for axis, length in enumerate(array.shape)]
    widest = array.shape.index(max(array.shape))
    neighbour = index_at[:widest] + [(index_at[widest] + 1) % array.shape[widest]] + index_at[widest + 1:]
    return array.at[tuple(index_at)].set(least).at[tuple(neighbour)].set(high)


def levels(stream_key, shape, cuts, low, high):
    loudness = 1.0
    for dim, blocks in cuts:
        draws = jax.random.uniform(jax.random.fold_in(jax.random.fold_in(stream_key, 6), dim), (blocks,), jnp.float32, low / len(cuts), high / len(cuts))
        loudness = loudness * jnp.repeat(jnp.exp(draws), shape[dim] // blocks).reshape((-1,) + (1,) * (len(shape) - 1 - dim))
    return loudness


def assign_block(key, own, number, rows, count, top, limit, lean):
    ranking = jax.random.permutation(key, count)
    packed, common = portions_of(count, rows * top, limit, lean, True), portions_of(count, rows * top, limit, lean, False)
    places = jnp.arange(count)

    def named(sizes, rotation):
        used = int((sizes > 0).sum())
        fixed = max(1, used // 4)
        moved = fixed + (places - fixed + rotation * (used - fixed)) % max(1, count - fixed)
        return jnp.zeros((count,), jnp.int32).at[ranking[jnp.where(places < fixed, places, moved)]].set(jnp.asarray(sizes, jnp.int32))

    sizes = jnp.where(number % 4 == 0, named(packed, number // 4), named(common, number - number // 4 - 1))
    mixed = jax.random.permutation(jax.random.fold_in(own, 3), count)
    donor, taker = mixed[0:count // 2 * 2:2], mixed[1:count // 2 * 2:2]
    margin = jnp.minimum(sizes[donor] - 1, limit - sizes[taker]) // 2
    margin = jnp.where((donor == ranking[0]) | (taker == ranking[0]) | (sizes[taker] == 0), 0, jnp.maximum(margin, 0))
    moved = jax.random.randint(jax.random.fold_in(own, 4), (count // 2,), 0, 1 << 20) % (margin + 1)
    sizes = sizes.at[donor].add(-moved).at[taker].add(moved)
    items = jnp.searchsorted(jnp.cumsum(sizes), jnp.arange(rows * top), side="right").astype(jnp.int32)
    table = items.reshape(top, rows).T
    table = table[jax.random.permutation(jax.random.fold_in(own, 1), rows)]
    rotation = jax.random.randint(jax.random.fold_in(own, 2), (rows, 1), 0, top)
    return jnp.take_along_axis(table, (jnp.arange(top)[None, :] + rotation) % top, axis=1)


def portions_of(number_of, total, most, slope, full):
    loads = [(1 << 20) // math.isqrt(standing ** slope) + 1 for standing in range(1, number_of + 1)]
    largest = most if full else min(most, max(-(-total // number_of), total * loads[0] // sum(loads)))
    least = 1 if total - largest >= number_of - 1 else 0
    holding, surplus = [largest] + [least] * (number_of - 1), total - largest - least * (number_of - 1)
    while surplus > 0:
        free = [i for i in range(1, number_of) if holding[i] < largest] or [i for i in range(1, number_of) if holding[i] < most]
        whole, budget = sum([loads[i] for i in free]), surplus
        for i in free:
            more = min(most - holding[i], max(1, budget * loads[i] // whole), surplus)
            holding[i] = holding[i] + more
            surplus = surplus - more
    return np.array(holding)


def noise(stream_key, shape, scale, reach, split=(), kind=jnp.bfloat16):
    array = scale * jax.random.normal(stream_key, shape, jnp.float32)
    if split:
        array = array * levels(stream_key, shape, split, -0.22, 0.18)
    return jnp.clip(array, -reach, reach).astype(kind)


def setup_inputs(seed: int = 0, part: int = 0) -> dict:
    key_of = jax.random.split(jax.random.key(seed), 14)
    part_keys = jax.random.split(jax.random.fold_in(key_of[13], part), 14)
    residual = noise(part_keys[0], (TOKENS, D), 0.3, 1.796875, ((0, 32),))
    queries = draw_queries(jax.random.fold_in(jax.random.fold_in(key_of[13], part), 71), part)
    key_new = noise(part_keys[2], (TOKENS, KVH * HD), 1.0, 6.0, ((0, 32),))
    value_new = noise(part_keys[3], (TOKENS, KVH * HD), 1.0, 6.0, ((0, 32),))
    key_cache = noise(part_keys[4], (TOKENS, WIN, KVH * HD), 1.0, 6.0, ((0, 32),))
    value_cache = noise(part_keys[5], (TOKENS, WIN, KVH * HD), 1.0, 6.0, ((0, 32),))
    lengths = with_ends(jax.random.randint(part_keys[6], (TOKENS,), 1, 4 * WIN + 1), jax.random.fold_in(part_keys[6], 1), 1, 4 * WIN).astype(jnp.int32)
    sink_logits = noise(key_of[7], (QH,), 1.5, 6.0, (), jnp.float32)
    norm_gain = jnp.clip(1.0 + 0.18 * jax.random.normal(key_of[8], (D,), jnp.float32), 0.1, 1.9)
    route_ids_keys = jax.random.split(jax.random.fold_in(part_keys[9], 1), TOKENS // (2 * TOK_DEV))
    route_ids_turns = jax.random.permutation(jax.random.fold_in(part_keys[9], 3), TOKENS // (2 * TOK_DEV))
    route_ids = jax.vmap(lambda own, number: assign_block(jax.random.fold_in(part_keys[9], 2), own, number, 2 * TOK_DEV, EXPERTS, TOPK, CAP, 2))(route_ids_keys, route_ids_turns).reshape((TOKENS, TOPK))
    route_logits = jnp.clip(jax.random.uniform(part_keys[10], (TOKENS, TOPK), jnp.float32, -1.0, 1.0) * levels(part_keys[10], (TOKENS, TOPK), ((0, 16),), -0.4, 0.0), -1.0, 1.0)
    up_weight = noise(key_of[11], (D, EXPERTS * FF), D ** -0.5, 0.109375, ((1, 32),))
    down_weight = noise(key_of[12], (EXPERTS * FF, D), FF ** -0.5, 0.15625, ((0, 32),))
    return dict(residual=residual, queries=queries, key_new=key_new, value_new=value_new, key_cache=key_cache, value_cache=value_cache, lengths=lengths, sink_logits=sink_logits, norm_gain=norm_gain, route_ids=route_ids, route_logits=route_logits, up_weight=up_weight, down_weight=down_weight)


def attention(queries, key_new, value_new, key_cache, value_cache, lengths, sink_logits):
    request_count = queries.shape[0]
    window = key_cache.shape[1]
    heads_kv = key_new.shape[1] // HD
    group_size = queries.shape[1] // (heads_kv * HD)
    query_heads = queries.astype(jnp.float32).reshape(request_count, heads_kv, group_size, HD)
    cached_keys = key_cache.astype(jnp.float32).reshape(request_count, window, heads_kv, HD)
    cached_values = value_cache.astype(jnp.float32).reshape(request_count, window, heads_kv, HD)
    fresh_key = key_new.astype(jnp.float32).reshape(request_count, heads_kv, HD)
    fresh_value = value_new.astype(jnp.float32).reshape(request_count, heads_kv, HD)
    score_scale = HD ** (-0.5)
    cached = jnp.einsum('tkgd,tskd->tkgs', query_heads, cached_keys) * score_scale
    fresh_score = jnp.einsum('tkgd,tkd->tkg', query_heads, fresh_key) * score_scale
    newest = lengths[:, None] - 1
    slot_index = jnp.arange(window, dtype=jnp.int32)[None, :]
    position = newest - jnp.mod(newest - slot_index, window)
    visible = (position >= 0) & (position >= lengths[:, None] - window + 1)
    cached = jnp.where(visible[:, None, None, :], cached, -1e+30)
    sink_logit = sink_logits.reshape(1, heads_kv, group_size)
    highest = jnp.maximum(jnp.maximum(lax.optimization_barrier(jnp.max(cached, -1)), fresh_score), sink_logit)
    weights = jnp.exp(cached - highest[..., None])
    fresh_weight = jnp.exp(fresh_score - highest)
    denominator = lax.optimization_barrier(jnp.sum(weights, -1)) + fresh_weight + jnp.exp(sink_logit - highest)
    cache_probs = (weights / denominator[..., None]).astype(jnp.bfloat16)
    fresh_prob = (fresh_weight / denominator).astype(jnp.bfloat16)
    context = jnp.einsum('tkgs,tskd->tkgd', cache_probs.astype(jnp.float32), cached_values)
    context = context + fresh_prob.astype(jnp.float32)[..., None] * fresh_value[:, :, None, :]
    return context.reshape(request_count, -1)

def reference(residual, queries, key_new, value_new, key_cache, value_cache, lengths, sink_logits, norm_gain, route_ids, route_logits, up_weight, down_weight):
    context = attention(queries, key_new, value_new, key_cache, value_cache, lengths, sink_logits)
    hidden_state = residual.astype(jnp.float32) + context
    normed = (hidden_state * lax.rsqrt(lax.optimization_barrier(jnp.mean(hidden_state * hidden_state, -1, keepdims=True)) + 1e-05) * norm_gain).astype(jnp.bfloat16)
    gate_weights = jax.nn.softmax(route_logits, axis=-1)
    request_count, pick_count = route_ids.shape
    blocks = N_EP
    block_ids = route_ids.reshape(blocks, -1)
    onehot = (block_ids[..., None] == jnp.arange(EXPERTS, dtype=jnp.int32)).astype(jnp.int32)
    earlier = jnp.cumsum(onehot, axis=1) - onehot
    slot_number = lax.optimization_barrier(jnp.sum(earlier * onehot, -1))
    slot_place = (jnp.arange(blocks, dtype=jnp.int32)[:, None] * CAP + slot_number).reshape(-1).astype(jnp.int32)
    expert_flat = route_ids.reshape(-1).astype(jnp.int32)
    token_flat = jnp.repeat(jnp.arange(request_count, dtype=jnp.int32), pick_count)
    index_table = jnp.zeros((EXPERTS, blocks * CAP), jnp.int32).at[expert_flat, slot_place].set(token_flat)
    gate_table = jnp.zeros((EXPERTS, blocks * CAP), jnp.float32).at[expert_flat, slot_place].set(gate_weights.reshape(-1))
    quarters = 2 * N_ROLE
    up_stack = up_weight.reshape(D, EXPERTS, FF).transpose(1, 0, 2)
    down_stack = down_weight.reshape(EXPERTS, quarters, HID_DEV, D)

    def expert_step(running, inputs):
        row_index, row_gate, up_block, down_block = inputs
        gathered = normed[row_index]
        activation = jax.nn.silu(jnp.dot(gathered, up_block, preferred_element_type=jnp.float32)).astype(jnp.bfloat16)
        split_act = activation.reshape(-1, quarters, HID_DEV).astype(jnp.float32)
        partials = jnp.einsum('rqh,qhd->rqd', split_act, down_block.astype(jnp.float32)).astype(jnp.bfloat16)
        summed = lax.optimization_barrier(jnp.sum(partials.astype(jnp.float32), axis=1)) * row_gate[:, None]
        return (running.at[row_index].add(summed), None)
    expert_out, _ = lax.scan(expert_step, jnp.zeros((request_count, D), jnp.float32), (index_table, gate_table, up_stack, down_stack))
    return (hidden_state + expert_out).astype(jnp.bfloat16)
```

```python
import functools

import jax
import jax.numpy as jnp
from jax import lax
from jax.experimental import pallas as pl
from jax.experimental.pallas import tpu as pltpu
from jax.sharding import PartitionSpec as P

HD = 64
LANES = 128
SLOTS = 8
MESH = pl.DeviceIdType.MESH
BF16 = jnp.bfloat16
F32 = jnp.float32


def iota(shape, dim):
    return lax.broadcasted_iota(jnp.int32, shape, dim)


def spread_queries(q_ref, wide_ref, group_size):
    rows, width = q_ref.shape
    heads = width // HD
    wide_ref[...] = jnp.zeros_like(wide_ref)
    kv_width = wide_ref.shape[2]
    for head in range(heads):
        tile, half = head // 2, head % 2
        size = min(LANES, width - tile * LANES)
        block = q_ref[:, tile * LANES : tile * LANES + size].astype(F32)
        if size < LANES:
            block = jnp.concatenate([block, jnp.zeros((rows, LANES - size), F32)], axis=1)
        kv = head // group_size
        if half != kv % 2:
            block = pltpu.roll(block, HD, 1)
        lane = iota(block.shape, 1)
        block = jnp.where((lane // HD) == (kv % 2), block, 0.0)
        start = (kv // 2) * LANES
        stop = min(start + LANES, kv_width)
        wide_ref[:, head, start:stop] = block[:, : stop - start]


def attend(wide_ref, kn_ref, vn_ref, k_ref, v_ref, len_ref, sink_ref, ctx_ref, group_size):
    requests, head_rows, kv_width = wide_ref.shape
    window = k_ref.shape[1]
    heads = sink_ref.shape[1]
    scale = HD ** (-0.5)
    eye = iota((head_rows, heads), 0) == iota((head_rows, heads), 1)
    sink = jnp.sum(jnp.where(eye, sink_ref[...], 0.0), axis=1, keepdims=True)
    own = (iota((head_rows, kv_width), 0) // group_size) == (iota((head_rows, kv_width), 1) // HD)
    slot = iota((1, window), 1)
    for t in range(requests):
        length = len_ref[t]
        newest = length - 1
        behind = lax.rem(newest, window) - slot
        behind = jnp.where(behind < 0, behind + window, behind)
        position = newest - behind
        visible = (position >= 0) & (position >= length - window + 1)
        q = wide_ref[t]
        scores = (
            lax.dot_general(
                q.astype(BF16), k_ref[t], (((1,), (1,)), ((), ())), preferred_element_type=F32
            )
            * scale
        )
        scores = jnp.where(visible, scores, -1e30)
        fresh = (
            jnp.sum(q * kn_ref[t : t + 1, :].astype(F32), axis=1, keepdims=True) * scale
        )
        highest = jnp.maximum(
            jnp.maximum(jnp.max(scores, axis=1, keepdims=True), fresh), sink
        )
        weights = jnp.exp(scores - highest)
        fresh_weight = jnp.exp(fresh - highest)
        total = jnp.sum(weights, axis=1, keepdims=True) + fresh_weight + jnp.exp(sink - highest)
        probs = (weights / total).astype(BF16)
        fresh_prob = (fresh_weight / total).astype(BF16).astype(F32)
        context = jnp.dot(probs, v_ref[t], preferred_element_type=F32)
        context = context + fresh_prob * vn_ref[t : t + 1, :].astype(F32)
        context = jnp.where(own, context, 0.0)
        folded = jnp.zeros((head_rows, LANES), F32)
        for start in range(0, kv_width, LANES):
            part = context[:, start : min(start + LANES, kv_width)]
            if part.shape[1] < LANES:
                part = jnp.concatenate(
                    [part, jnp.zeros((head_rows, LANES - part.shape[1]), F32)], axis=1
                )
            folded = folded + part
        ctx_ref[t] = folded + pltpu.roll(folded, HD, 1)


def kernel(
    n,
    capacity,
    half,
    q_ref,
    res_ref,
    kn_ref,
    vn_ref,
    len_ref,
    sink_ref,
    gain_ref,
    ids_ref,
    logit_ref,
    k_hbm,
    v_hbm,
    up_hbm,
    down_hbm,
    out_ref,
    k_ref,
    v_ref,
    up_ref,
    down_ref,
    wide_ref,
    ctx_ref,
    hid_ref,
    norm_ref,
    rows_ref,
    ids_pad,
    logit_pad,
    packed_ref,
    recv_ref,
    act_ref,
    down_half,
    down_peer,
    sent_ref,
    back_ref,
    mix_ref,
    mix_peer,
    load_sem,
    one_send,
    one_recv,
    go_send,
    go_recv,
    fwd_send,
    fwd_recv,
    ret_send,
    ret_recv,
):
    me = lax.axis_index("ep")
    core = lax.axis_index("role")
    group = lax.axis_index("groups")
    peer = (group, me, 1 - core)
    rows, width = res_ref.shape
    heads = width // HD
    experts = n // 2
    group_size = heads // (kn_ref.shape[1] // HD)
    depth = down_ref.shape[0]

    loads = [
        pltpu.make_async_copy(src, dst, load_sem.at[i])
        for i, (src, dst) in enumerate(
            ((k_hbm, k_ref), (v_hbm, v_ref), (down_hbm, down_ref), (up_hbm, up_ref))
        )
    ]
    for load in loads:
        load.start()

    recv_ref[...] = jnp.zeros_like(recv_ref)
    back_ref[...] = jnp.zeros_like(back_ref)

    barrier = pltpu.get_barrier_semaphore()
    pl.semaphore_signal(barrier, inc=1, device_id=peer, device_id_type=MESH)

    @pl.loop(1, n)
    def _(step):
        other = lax.rem(me + step, n)
        pl.semaphore_signal(barrier, inc=1, device_id=(group, other, core), device_id_type=MESH)

    token_rows = 2 * SLOTS
    ids_pad[...] = jnp.full(ids_pad.shape, -1, jnp.int32)
    logit_pad[...] = jnp.zeros(logit_pad.shape, F32)
    for side in range(2):
        ids_pad[side * SLOTS : side * SLOTS + rows, :] = ids_ref[side * rows : (side + 1) * rows, :]
        logit_pad[side * SLOTS : side * SLOTS + rows, :] = logit_ref[
            side * rows : (side + 1) * rows, :
        ]
    ids = ids_pad[...]
    logits = logit_pad[...]
    gates = jnp.exp(logits - jnp.max(logits, axis=1, keepdims=True))
    gates = gates / jnp.sum(gates, axis=1, keepdims=True)
    earlier = (iota((token_rows, token_rows), 1) < iota((token_rows, token_rows), 0)).astype(F32)

    def tables(columns, per_expert):
        shape = (token_rows, columns)
        expert = iota(shape, 1) // per_expert
        slot = lax.rem(iota(shape, 1), SLOTS)
        hot = jnp.zeros(shape, F32)
        gate = jnp.zeros(shape, F32)
        for pick in range(ids.shape[1]):
            named = ids[:, pick : pick + 1] == expert
            hot = hot + jnp.where(named, 1.0, 0.0)
            gate = gate + jnp.where(named, gates[:, pick : pick + 1], 0.0)
        place = jnp.dot(earlier.astype(BF16), hot.astype(BF16), preferred_element_type=F32)
        chosen = jnp.where(place == slot.astype(F32), hot, 0.0)
        return chosen, gate * chosen

    spread_queries(q_ref, wide_ref, group_size)
    loads[0].wait()
    loads[1].wait()
    attend(wide_ref, kn_ref, vn_ref, k_ref, v_ref, len_ref, sink_ref, ctx_ref, group_size)
    hid_ref[...] = jnp.zeros_like(hid_ref)
    for tile in range((heads + 1) // 2):
        first = ctx_ref[:, 2 * tile, :]
        if 2 * tile + 1 < heads:
            second = ctx_ref[:, 2 * tile + 1, :]
        else:
            second = jnp.zeros_like(first)
        size = min(LANES, width - tile * LANES)
        both = jnp.where(iota(first.shape, 1) < HD, first, second)[:, :size]
        columns = slice(tile * LANES, tile * LANES + size)
        hid_ref[0:rows, columns] = both + res_ref[:, columns].astype(F32)
    hidden = hid_ref[...]
    inverse = lax.rsqrt(jnp.sum(hidden * hidden, axis=1, keepdims=True) / width + 1e-05)
    norm_ref[0] = (hidden[:, :half] * inverse * gain_ref[:, :half]).astype(BF16)
    norm_ref[1] = jnp.zeros(norm_ref.shape[1:], BF16)
    norm_ref[1, :, : width - half] = (
        hidden[:, half:width] * inverse * gain_ref[:, half:]
    ).astype(BF16)

    pl.semaphore_wait(barrier, n)

    def to_peer(src, dst, number):
        return pltpu.make_async_remote_copy(
            src_ref=src,
            dst_ref=dst,
            send_sem=one_send.at[number],
            recv_sem=one_recv.at[number],
            device_id=peer,
            device_id_type=MESH,
        )

    swap_rows = to_peer(norm_ref.at[1 - core], rows_ref.at[core], 0)
    swap_rows.start()
    rows_ref[core] = norm_ref[core]

    loads[2].wait()
    down_half[0] = down_ref[:, :half]
    down_half[1] = jnp.zeros(down_half.shape[1:], BF16)
    down_half[1, :, : width - half] = down_ref[:, half:]

    send_table, _ = tables(max(experts * SLOTS, LANES), SLOTS)
    send_table = send_table.T[: experts * SLOTS].astype(BF16)
    swap_rows.wait()
    token_block = rows_ref[...].astype(F32).reshape(token_rows, half).astype(BF16)
    packed = jnp.dot(send_table, token_block, preferred_element_type=F32)
    packed_ref[...] = packed.reshape(experts, SLOTS, half).astype(BF16)

    used = pl.ds(0, capacity)

    def go(step):
        other = lax.rem(me + step, n)
        return pltpu.make_async_remote_copy(
            src_ref=packed_ref.at[other // 2, used],
            dst_ref=recv_ref.at[core, me, used],
            send_sem=go_send.at[other],
            recv_sem=go_recv.at[me],
            device_id=(group, other, core),
            device_id_type=MESH,
        )

    def come(step, buffer, send_sem, recv_sem):
        source = lax.rem(me + n - step, n)
        return source, pltpu.make_async_remote_copy(
            src_ref=buffer,
            dst_ref=buffer,
            send_sem=send_sem.at[source],
            recv_sem=recv_sem.at[source],
            device_id=peer,
            device_id_type=MESH,
        )

    @pl.loop(1, n)
    def _(step):
        go(step).start()

    swap_down = to_peer(down_half.at[1 - core], down_peer, 1)
    swap_down.start()

    def forward(src, source):
        return pltpu.make_async_remote_copy(
            src_ref=src,
            dst_ref=recv_ref.at[core, source, used],
            send_sem=fwd_send.at[source],
            recv_sem=fwd_recv.at[source],
            device_id=peer,
            device_id_type=MESH,
        )

    recv_ref[core, me] = packed_ref[me // 2]
    forward(packed_ref.at[me // 2, used], me).start()

    @pl.loop(1, n)
    def _(step):
        source = lax.rem(me + n - step, n)
        block = recv_ref.at[core, source, used]
        come(step, block, go_send, go_recv)[1].wait_recv()
        forward(block, source).start()

    @pl.loop(0, n)
    def _(source):
        block = recv_ref.at[1 - core, source, used]
        pltpu.make_async_remote_copy(
            src_ref=block,
            dst_ref=block,
            send_sem=fwd_send.at[source],
            recv_sem=fwd_recv.at[source],
            device_id=peer,
            device_id_type=MESH,
        ).wait_recv()

    loads[3].wait()
    chunk = min(n, 16)
    chunk_rows = chunk * SLOTS

    @pl.loop(0, n // chunk)
    def _(part):
        blocks = pl.ds(part * chunk, chunk)
        low = recv_ref[0, blocks].astype(F32).reshape(chunk_rows, half).astype(BF16)
        high = recv_ref[1, blocks].astype(F32).reshape(chunk_rows, half).astype(BF16)
        value = jnp.dot(low, up_ref[:half, :], preferred_element_type=F32) + jnp.dot(
            high[:, : width - half], up_ref[half:, :], preferred_element_type=F32
        )
        value = value / (1.0 + jnp.exp(-value))
        act_ref[core, pl.ds(pl.multiple_of(part * chunk_rows, chunk_rows), chunk_rows), :] = (
            value.astype(BF16)
        )

    swap_act = to_peer(act_ref.at[core], act_ref.at[core], 2)
    swap_act.start()
    swap_down.wait()
    swap_act.wait()

    @pl.loop(0, n // chunk)
    def _(part):
        blocks = pl.ds(part * chunk, chunk)
        place = pl.ds(pl.multiple_of(part * chunk_rows, chunk_rows), chunk_rows)
        value = jnp.dot(
            act_ref[core, place, :], down_half[core], preferred_element_type=F32
        ) + jnp.dot(act_ref[1 - core, place, :], down_peer[...], preferred_element_type=F32)
        sent_ref[blocks] = value.reshape(chunk, SLOTS, half).astype(BF16)

    def give_back(step):
        other = lax.rem(me + step, n)
        return pltpu.make_async_remote_copy(
            src_ref=sent_ref.at[other, used],
            dst_ref=back_ref.at[me, used],
            send_sem=ret_send.at[other],
            recv_sem=ret_recv.at[me],
            device_id=(group, other, core),
            device_id_type=MESH,
        )

    @pl.loop(1, n)
    def _(step):
        give_back(step).start()

    back_ref[me] = sent_ref[me]
    _, mixing = tables(n * SLOTS, 2 * SLOTS)
    coarse = mixing.astype(BF16)
    fine = (mixing - coarse.astype(F32)).astype(BF16)

    @pl.loop(1, n)
    def _(step):
        go(step).wait_send()

    @pl.loop(0, n)
    def _(source):
        forward(recv_ref.at[core, source, used], source).wait_send()

    @pl.loop(1, n)
    def _(step):
        source = lax.rem(me + n - step, n)
        come(step, back_ref.at[source, used], ret_send, ret_recv)[1].wait_recv()

    returned = back_ref[...].astype(F32).reshape(n * SLOTS, half).astype(BF16)
    mixed = jnp.dot(coarse, returned, preferred_element_type=F32) + jnp.dot(
        fine, returned, preferred_element_type=F32
    )
    mix_ref[...] = mixed.reshape(2, SLOTS, half).astype(BF16)
    swap_mix = to_peer(mix_ref.at[1 - core], mix_peer, 3)
    swap_mix.start()
    mine = jnp.where(core == 0, mixed[:SLOTS], mixed[SLOTS:])

    @pl.loop(1, n)
    def _(step):
        give_back(step).wait_send()

    swap_mix.wait()
    theirs = mix_peer[...].astype(F32)
    low = jnp.where(core == 0, mine, theirs)
    high = jnp.where(core == 0, theirs, mine)
    out_ref[:, :half] = (hid_ref[:, :half] + low)[:rows].astype(BF16)
    out_ref[:, half:] = (hid_ref[:, half:width] + high[:, : width - half])[:rows].astype(BF16)


def local(
    residual,
    queries,
    key_new,
    value_new,
    key_cache,
    value_cache,
    lengths,
    sink_logits,
    norm_gain,
    route_ids,
    route_logits,
    up_weight,
    down_weight,
):
    n = lax.axis_size("ep")
    experts = n // 2
    pair_count, pick_count = route_ids.shape
    capacity = min(pair_count, max(2, (pair_count * pick_count + experts - 1) // experts))
    rows, width = residual.shape
    half = -(-width // (4 * LANES)) * 2 * LANES
    heads = width // HD
    head_rows = -(-heads // 8) * 8
    depth = up_weight.shape[1]
    vmem = pl.BlockSpec(memory_space=pltpu.VMEM)
    smem = pl.BlockSpec(memory_space=pltpu.SMEM)
    anywhere = pl.BlockSpec(memory_space=pl.ANY)
    dma = pltpu.SemaphoreType.DMA
    return pl.pallas_call(
        functools.partial(kernel, n, capacity, half),
        out_shape=jax.ShapeDtypeStruct((rows, width), BF16),
        in_specs=[vmem] * 4 + [smem] + [vmem] * 4 + [anywhere] * 4,
        out_specs=vmem,
        scratch_shapes=[
            pltpu.VMEM(key_cache.shape, BF16),
            pltpu.VMEM(value_cache.shape, BF16),
            pltpu.VMEM(up_weight.shape, BF16),
            pltpu.VMEM(down_weight.shape, BF16),
            pltpu.VMEM((rows, head_rows, key_new.shape[1]), F32),
            pltpu.VMEM((rows, head_rows, LANES), F32),
            pltpu.VMEM((SLOTS, 2 * half), F32),
            pltpu.VMEM((2, SLOTS, half), BF16),
            pltpu.VMEM((2, SLOTS, half), BF16),
            pltpu.VMEM((2 * SLOTS, pick_count), jnp.int32),
            pltpu.VMEM((2 * SLOTS, pick_count), F32),
            pltpu.VMEM((experts, SLOTS, half), BF16),
            pltpu.VMEM((2, n, SLOTS, half), BF16),
            pltpu.VMEM((2, n * SLOTS, depth), BF16),
            pltpu.VMEM((2, depth, half), BF16),
            pltpu.VMEM((depth, half), BF16),
            pltpu.VMEM((n, SLOTS, half), BF16),
            pltpu.VMEM((n, SLOTS, half), BF16),
            pltpu.VMEM((2, SLOTS, half), BF16),
            pltpu.VMEM((SLOTS, half), BF16),
            dma((4,)),
            dma((4,)),
            dma((4,)),
            dma((n,)),
            dma((n,)),
            dma((n,)),
            dma((n,)),
            dma((n,)),
            dma((n,)),
        ],
        compiler_params=pltpu.CompilerParams(
            collective_id=0, has_side_effects=True, vmem_limit_bytes=60 * 1024 * 1024
        ),
    )(
        queries,
        residual,
        key_new,
        value_new,
        lengths,
        sink_logits.reshape(1, -1),
        norm_gain.reshape(1, -1),
        route_ids,
        route_logits,
        key_cache,
        value_cache,
        up_weight,
        down_weight,
    )


def solution(mesh):
    placed = (
        P(("groups", "ep", "role"), None),
        P(("groups", "ep", "role"), None),
        P(("groups", "ep", "role"), None),
        P(("groups", "ep", "role"), None),
        P(("groups", "ep", "role"), None, None),
        P(("groups", "ep", "role"), None, None),
        P(("groups", "ep", "role")),
        P(),
        P(),
        P(("groups", "ep"), None),
        P(("groups", "ep"), None),
        P(None, ("ep", "role")),
        P(("ep", "role"), None),
    )
    return jax.shard_map(
        local,
        mesh=mesh,
        in_specs=placed,
        out_specs=P(("groups", "ep", "role"), None),
        check_vma=False,
    )
```

```python
import functools

import jax
import jax.numpy as jnp
from jax import lax
from jax.experimental import pallas as pl
from jax.experimental.pallas import tpu as pltpu
from jax.sharding import PartitionSpec as P

HD = 64
LANES = 128
SLOTS = 8
MESH = pl.DeviceIdType.MESH
BF16 = jnp.bfloat16
F32 = jnp.float32


def iota(shape, dim):
    return lax.broadcasted_iota(jnp.int32, shape, dim)


def dot_nt(a, b):
    return lax.dot_general(a, b, (((1,), (1,)), ((), ())), preferred_element_type=F32)


def spread_queries(q_ref, wide_ref, group_size):
    rows, width = q_ref.shape
    heads = width // HD
    wide_ref[...] = jnp.zeros_like(wide_ref)
    kv_width = wide_ref.shape[2]
    for head in range(heads):
        tile, half = head // 2, head % 2
        size = min(LANES, width - tile * LANES)
        block = q_ref[:, tile * LANES : tile * LANES + size].astype(F32)
        if size < LANES:
            block = jnp.concatenate([block, jnp.zeros((rows, LANES - size), F32)], axis=1)
        kv = head // group_size
        if half != kv % 2:
            block = pltpu.roll(block, HD, 1)
        lane = iota(block.shape, 1)
        block = jnp.where((lane // HD) == (kv % 2), block, 0.0)
        start = (kv // 2) * LANES
        stop = min(start + LANES, kv_width)
        wide_ref[:, head, start:stop] = block[:, : stop - start]


def attend(wide_ref, kn_ref, vn_ref, k_ref, v_ref, len_ref, sink_ref, ctx_ref, group_size):
    requests, head_rows, kv_width = wide_ref.shape
    window = k_ref.shape[2]
    heads = sink_ref.shape[1]
    scale = HD ** (-0.5)
    eye = iota((head_rows, heads), 0) == iota((head_rows, heads), 1)
    sink = jnp.sum(jnp.where(eye, sink_ref[...], 0.0), axis=1, keepdims=True)
    own = (iota((head_rows, kv_width), 0) // group_size) == (iota((head_rows, kv_width), 1) // HD)
    slot = iota((1, window), 1)
    for t in range(requests):
        length = len_ref[t]
        newest = length - 1
        behind = lax.rem(newest, window) - slot
        behind = jnp.where(behind < 0, behind + window, behind)
        position = newest - behind
        visible = (position >= 0) & (position >= length - window + 1)
        q = wide_ref[t]
        scores = (
            jnp.dot(q.astype(BF16), k_ref[t], preferred_element_type=F32) * scale
        )
        scores = jnp.where(visible, scores, -1e30)
        fresh = (
            jnp.sum(q * kn_ref[t : t + 1, :].astype(F32), axis=1, keepdims=True) * scale
        )
        highest = jnp.maximum(
            jnp.maximum(jnp.max(scores, axis=1, keepdims=True), fresh), sink
        )
        weights = jnp.exp(scores - highest)
        fresh_weight = jnp.exp(fresh - highest)
        total = jnp.sum(weights, axis=1, keepdims=True) + fresh_weight + jnp.exp(sink - highest)
        probs = (weights / total).astype(BF16)
        fresh_prob = (fresh_weight / total).astype(BF16).astype(F32)
        context = dot_nt(probs, v_ref[t])
        context = context + fresh_prob * vn_ref[t : t + 1, :].astype(F32)
        context = jnp.where(own, context, 0.0)
        folded = jnp.zeros((head_rows, LANES), F32)
        for start in range(0, kv_width, LANES):
            part = context[:, start : min(start + LANES, kv_width)]
            if part.shape[1] < LANES:
                part = jnp.concatenate(
                    [part, jnp.zeros((head_rows, LANES - part.shape[1]), F32)], axis=1
                )
            folded = folded + part
        ctx_ref[t] = folded + pltpu.roll(folded, HD, 1)


def kernel(
    n,
    capacity,
    half,
    q_ref,
    res_ref,
    kn_ref,
    vn_ref,
    len_ref,
    sink_ref,
    gain_ref,
    ids_ref,
    logit_ref,
    k_hbm,
    v_hbm,
    up_hbm,
    down_hbm,
    out_ref,
    k_ref,
    v_ref,
    up_ref,
    down_ref,
    wide_ref,
    ctx_ref,
    hid_ref,
    norm_ref,
    rows_ref,
    ids_wide,
    ids_pad,
    logit_wide,
    logit_pad,
    packed_ref,
    recv_ref,
    act_ref,
    down_half,
    down_peer,
    sent_ref,
    back_ref,
    mix_ref,
    mix_peer,
    load_sem,
    one_send,
    one_recv,
    go_send,
    go_recv,
    fwd_send,
    fwd_recv,
    ret_send,
    ret_recv,
):
    me = lax.axis_index("ep")
    core = lax.axis_index("role")
    group = lax.axis_index("groups")
    peer = (group, me, 1 - core)
    rows, width = res_ref.shape
    heads = width // HD
    experts = n // 2
    group_size = heads // (kn_ref.shape[1] // HD)

    loads = [
        pltpu.make_async_copy(src, dst, load_sem.at[i])
        for i, (src, dst) in enumerate(
            ((k_hbm, k_ref), (v_hbm, v_ref), (down_hbm, down_ref), (up_hbm, up_ref))
        )
    ]
    for load in loads:
        load.start()

    back_ref[...] = jnp.zeros_like(back_ref)

    barrier = pltpu.get_barrier_semaphore()
    pl.semaphore_signal(barrier, inc=1, device_id=peer, device_id_type=MESH)

    @pl.loop(1, n)
    def _(step):
        other = lax.rem(me + step, n)
        pl.semaphore_signal(barrier, inc=1, device_id=(group, other, core), device_id_type=MESH)

    token_rows = 2 * SLOTS
    picks = ids_ref.shape[0]

    def by_token(src, wide, tall, fill):
        wide[...] = jnp.full(wide.shape, fill, wide.dtype)
        wide[:picks, : 2 * rows] = src[...]
        turned = wide[...].T
        tall[...] = jnp.full(tall.shape, fill, tall.dtype)
        for side in range(2):
            tall[side * SLOTS : side * SLOTS + rows, :] = turned[
                side * rows : (side + 1) * rows, :
            ]
        return tall[:, :picks]

    ids = by_token(ids_ref, ids_wide, ids_pad, -1)
    logits = by_token(logit_ref, logit_wide, logit_pad, 0)
    gates = jnp.exp(logits - jnp.max(logits, axis=1, keepdims=True))
    gates = gates / jnp.sum(gates, axis=1, keepdims=True)
    earlier = (iota((token_rows, token_rows), 1) < iota((token_rows, token_rows), 0)).astype(F32)

    def tables(columns, per_expert):
        shape = (token_rows, columns)
        expert = iota(shape, 1) // per_expert
        slot = lax.rem(iota(shape, 1), SLOTS)
        hot = jnp.zeros(shape, F32)
        gate = jnp.zeros(shape, F32)
        for pick in range(ids.shape[1]):
            named = ids[:, pick : pick + 1] == expert
            hot = hot + jnp.where(named, 1.0, 0.0)
            gate = gate + jnp.where(named, gates[:, pick : pick + 1], 0.0)
        place = jnp.dot(earlier.astype(BF16), hot.astype(BF16), preferred_element_type=F32)
        chosen = jnp.where(place == slot.astype(F32), hot, 0.0)
        return chosen, gate * chosen

    spread_queries(q_ref, wide_ref, group_size)
    loads[0].wait()
    loads[1].wait()
    attend(wide_ref, kn_ref, vn_ref, k_ref, v_ref, len_ref, sink_ref, ctx_ref, group_size)
    hid_ref[...] = jnp.zeros_like(hid_ref)
    for tile in range((heads + 1) // 2):
        first = ctx_ref[:, 2 * tile, :]
        if 2 * tile + 1 < heads:
            second = ctx_ref[:, 2 * tile + 1, :]
        else:
            second = jnp.zeros_like(first)
        size = min(LANES, width - tile * LANES)
        both = jnp.where(iota(first.shape, 1) < HD, first, second)[:, :size]
        columns = slice(tile * LANES, tile * LANES + size)
        hid_ref[0:rows, columns] = both + res_ref[:, columns].astype(F32)
    hidden = hid_ref[...]
    inverse = lax.rsqrt(jnp.sum(hidden * hidden, axis=1, keepdims=True) / width + 1e-05)
    gain = gain_ref[...].reshape(1, width)
    norm_ref[0] = (hidden[:, :half] * inverse * gain[:, :half]).astype(BF16)
    norm_ref[1] = jnp.zeros(norm_ref.shape[1:], BF16)
    norm_ref[1, :, : width - half] = (
        hidden[:, half:width] * inverse * gain[:, half:]
    ).astype(BF16)

    pl.semaphore_wait(barrier, n)

    def to_peer(src, dst, number):
        return pltpu.make_async_remote_copy(
            src_ref=src,
            dst_ref=dst,
            send_sem=one_send.at[number],
            recv_sem=one_recv.at[number],
            device_id=peer,
            device_id_type=MESH,
        )

    swap_rows = to_peer(norm_ref.at[1 - core], rows_ref.at[core], 0)
    swap_rows.start()
    rows_ref[core] = norm_ref[core]

    loads[2].wait()
    down_half[0] = down_ref[:, :half]
    down_half[1] = jnp.zeros(down_half.shape[1:], BF16)
    down_half[1, :, : width - half] = down_ref[:, half:]

    send_table, _ = tables(max(experts * SLOTS, LANES), SLOTS)
    send_table = send_table.T[: experts * SLOTS].astype(BF16)
    swap_rows.wait()
    token_block = rows_ref[...].astype(F32).reshape(token_rows, half).astype(BF16)
    packed = jnp.dot(send_table, token_block, preferred_element_type=F32)
    packed_ref[...] = packed.reshape(experts, SLOTS, half).astype(BF16)

    used = pl.ds(0, capacity)

    def go(step):
        other = lax.rem(me + step, n)
        return pltpu.make_async_remote_copy(
            src_ref=packed_ref.at[other // 2, used],
            dst_ref=recv_ref.at[core, me, used],
            send_sem=go_send.at[other],
            recv_sem=go_recv.at[me],
            device_id=(group, other, core),
            device_id_type=MESH,
        )

    def come(step, buffer, send_sem, recv_sem):
        source = lax.rem(me + n - step, n)
        return source, pltpu.make_async_remote_copy(
            src_ref=buffer,
            dst_ref=buffer,
            send_sem=send_sem.at[source],
            recv_sem=recv_sem.at[source],
            device_id=peer,
            device_id_type=MESH,
        )

    @pl.loop(1, n)
    def _(step):
        go(step).start()

    swap_down = to_peer(down_half.at[1 - core], down_peer, 1)
    swap_down.start()

    def forward(src, source):
        return pltpu.make_async_remote_copy(
            src_ref=src,
            dst_ref=recv_ref.at[core, source, used],
            send_sem=fwd_send.at[source],
            recv_sem=fwd_recv.at[source],
            device_id=peer,
            device_id_type=MESH,
        )

    recv_ref[core, me] = packed_ref[me // 2]
    forward(packed_ref.at[me // 2, used], me).start()

    @pl.loop(1, n)
    def _(step):
        source = lax.rem(me + n - step, n)
        block = recv_ref.at[core, source, used]
        come(step, block, go_send, go_recv)[1].wait_recv()
        forward(block, source).start()

    @pl.loop(0, n)
    def _(source):
        block = recv_ref.at[1 - core, source, used]
        pltpu.make_async_remote_copy(
            src_ref=block,
            dst_ref=block,
            send_sem=fwd_send.at[source],
            recv_sem=fwd_recv.at[source],
            device_id=peer,
            device_id_type=MESH,
        ).wait_recv()

    loads[3].wait()
    chunk = min(n, 16)
    chunk_rows = chunk * SLOTS

    @pl.loop(0, n // chunk)
    def _(part):
        blocks = pl.ds(part * chunk, chunk)
        low = recv_ref[0, blocks].astype(F32).reshape(chunk_rows, half).astype(BF16)
        high = recv_ref[1, blocks].astype(F32).reshape(chunk_rows, half).astype(BF16)
        value = dot_nt(low, up_ref[:, :half]) + dot_nt(high[:, : width - half], up_ref[:, half:])
        value = value / (1.0 + jnp.exp(-value))
        act_ref[core, pl.ds(pl.multiple_of(part * chunk_rows, chunk_rows), chunk_rows), :] = (
            value.astype(BF16)
        )

    swap_act = to_peer(act_ref.at[core], act_ref.at[core], 2)
    swap_act.start()
    swap_down.wait()
    swap_act.wait()

    @pl.loop(0, n // chunk)
    def _(part):
        blocks = pl.ds(part * chunk, chunk)
        place = pl.ds(pl.multiple_of(part * chunk_rows, chunk_rows), chunk_rows)
        value = jnp.dot(
            act_ref[core, place, :], down_half[core], preferred_element_type=F32
        ) + jnp.dot(act_ref[1 - core, place, :], down_peer[...], preferred_element_type=F32)
        sent_ref[blocks] = value.reshape(chunk, SLOTS, half).astype(BF16)

    def give_back(step):
        other = lax.rem(me + step, n)
        return pltpu.make_async_remote_copy(
            src_ref=sent_ref.at[other, used],
            dst_ref=back_ref.at[me, used],
            send_sem=ret_send.at[other],
            recv_sem=ret_recv.at[me],
            device_id=(group, other, core),
            device_id_type=MESH,
        )

    @pl.loop(1, n)
    def _(step):
        give_back(step).start()

    back_ref[me] = sent_ref[me]
    _, mixing = tables(n * SLOTS, 2 * SLOTS)
    coarse = mixing.astype(BF16)
    fine = (mixing - coarse.astype(F32)).astype(BF16)

    @pl.loop(1, n)
    def _(step):
        go(step).wait_send()

    @pl.loop(0, n)
    def _(source):
        forward(recv_ref.at[core, source, used], source).wait_send()

    @pl.loop(1, n)
    def _(step):
        source = lax.rem(me + n - step, n)
        come(step, back_ref.at[source, used], ret_send, ret_recv)[1].wait_recv()

    returned = back_ref[...].astype(F32).reshape(n * SLOTS, half).astype(BF16)
    mixed = jnp.dot(coarse, returned, preferred_element_type=F32) + jnp.dot(
        fine, returned, preferred_element_type=F32
    )
    mix_ref[...] = mixed.reshape(2, SLOTS, half).astype(BF16)
    swap_mix = to_peer(mix_ref.at[1 - core], mix_peer, 3)
    swap_mix.start()
    mine = jnp.where(core == 0, mixed[:SLOTS], mixed[SLOTS:])

    @pl.loop(1, n)
    def _(step):
        give_back(step).wait_send()

    swap_mix.wait()
    theirs = mix_peer[...].astype(F32)
    low = jnp.where(core == 0, mine, theirs)
    high = jnp.where(core == 0, theirs, mine)
    out_ref[:, :half] = (hid_ref[:, :half] + low)[:rows]
    out_ref[:, half:] = (hid_ref[:, half:width] + high[:, : width - half])[:rows]


def local(
    residual,
    queries,
    key_new,
    value_new,
    key_cache,
    value_cache,
    lengths,
    sink_logits,
    norm_gain,
    route_ids,
    route_logits,
    up_weight,
    down_weight,
):
    n = lax.axis_size("ep")
    experts = n // 2
    pair_count, pick_count = route_ids.shape
    capacity = min(pair_count, max(2, (pair_count * pick_count + experts - 1) // experts))
    rows, width = residual.shape
    half = -(-width // (4 * LANES)) * 2 * LANES
    heads = width // HD
    head_rows = -(-heads // 8) * 8
    depth = up_weight.shape[1]
    vmem = pl.BlockSpec(memory_space=pltpu.VMEM)
    smem = pl.BlockSpec(memory_space=pltpu.SMEM)
    anywhere = pl.BlockSpec(memory_space=pl.ANY)
    dma = pltpu.SemaphoreType.DMA
    return pl.pallas_call(
        functools.partial(kernel, n, capacity, half),
        out_shape=jax.ShapeDtypeStruct((rows, width), F32),
        in_specs=[vmem] * 4 + [smem] + [vmem] * 4 + [anywhere] * 4,
        out_specs=vmem,
        scratch_shapes=[
            pltpu.VMEM((rows, key_cache.shape[2], key_cache.shape[1]), BF16),
            pltpu.VMEM((rows, key_cache.shape[2], key_cache.shape[1]), BF16),
            pltpu.VMEM((depth, width), BF16),
            pltpu.VMEM(down_weight.shape, BF16),
            pltpu.VMEM((rows, head_rows, key_new.shape[1]), F32),
            pltpu.VMEM((rows, head_rows, LANES), F32),
            pltpu.VMEM((SLOTS, 2 * half), F32),
            pltpu.VMEM((2, SLOTS, half), BF16),
            pltpu.VMEM((2, SLOTS, half), BF16),
            pltpu.VMEM((8, LANES), jnp.int32),
            pltpu.VMEM((2 * SLOTS, 8), jnp.int32),
            pltpu.VMEM((8, LANES), F32),
            pltpu.VMEM((2 * SLOTS, 8), F32),
            pltpu.VMEM((experts, SLOTS, half), BF16),
            pltpu.VMEM((2, n, SLOTS, half), BF16),
            pltpu.VMEM((2, n * SLOTS, depth), BF16),
            pltpu.VMEM((2, depth, half), BF16),
            pltpu.VMEM((depth, half), BF16),
            pltpu.VMEM((n, SLOTS, half), BF16),
            pltpu.VMEM((n, SLOTS, half), BF16),
            pltpu.VMEM((2, SLOTS, half), BF16),
            pltpu.VMEM((SLOTS, half), BF16),
            dma((4,)),
            dma((4,)),
            dma((4,)),
            dma((n,)),
            dma((n,)),
            dma((n,)),
            dma((n,)),
            dma((n,)),
            dma((n,)),
        ],
        compiler_params=pltpu.CompilerParams(
            collective_id=0, has_side_effects=True, vmem_limit_bytes=60 * 1024 * 1024
        ),
    )(
        queries,
        residual,
        key_new,
        value_new,
        lengths,
        sink_logits.reshape(1, -1),
        norm_gain,
        route_ids.T,
        route_logits.T,
        jnp.swapaxes(key_cache, 1, 2),
        jnp.swapaxes(value_cache, 1, 2),
        up_weight.T,
        down_weight,
    ).astype(BF16)


def solution(mesh):
    placed = (
        P(("groups", "ep", "role"), None),
        P(("groups", "ep", "role"), None),
        P(("groups", "ep", "role"), None),
        P(("groups", "ep", "role"), None),
        P(("groups", "ep", "role"), None, None),
        P(("groups", "ep", "role"), None, None),
        P(("groups", "ep", "role")),
        P(),
        P(),
        P(("groups", "ep"), None),
        P(("groups", "ep"), None),
        P(None, ("ep", "role")),
        P(("ep", "role"), None),
    )
    return jax.shard_map(
        local,
        mesh=mesh,
        in_specs=placed,
        out_specs=P(("groups", "ep", "role"), None),
        check_vma=False,
    )
```

```python
import functools

import jax
import jax.numpy as jnp
from jax import lax
from jax.experimental import pallas as pl
from jax.experimental.pallas import tpu as pltpu
from jax.sharding import PartitionSpec as P

HD = 64
LANES = 128
SLOTS = 8
MESH = pl.DeviceIdType.MESH
BF16 = jnp.bfloat16
F32 = jnp.float32


def iota(shape, dim):
    return lax.broadcasted_iota(jnp.int32, shape, dim)


def dot_nt(a, b):
    return lax.dot_general(a, b, (((1,), (1,)), ((), ())), preferred_element_type=F32)


def spread_queries(q_ref, wide_ref, group_size):
    rows, width = q_ref.shape
    heads = width // HD
    wide_ref[...] = jnp.zeros_like(wide_ref)
    kv_width = wide_ref.shape[2]
    for head in range(heads):
        tile, half = head // 2, head % 2
        size = min(LANES, width - tile * LANES)
        block = q_ref[:, tile * LANES : tile * LANES + size].astype(F32)
        if size < LANES:
            block = jnp.concatenate([block, jnp.zeros((rows, LANES - size), F32)], axis=1)
        kv = head // group_size
        if half != kv % 2:
            block = pltpu.roll(block, HD, 1)
        lane = iota(block.shape, 1)
        block = jnp.where((lane // HD) == (kv % 2), block, 0.0)
        start = (kv // 2) * LANES
        stop = min(start + LANES, kv_width)
        wide_ref[:, head, start:stop] = block[:, : stop - start]


def attend(wide_ref, kn_ref, vn_ref, k_ref, v_ref, len_ref, sink_ref, ctx_ref, group_size):
    requests, head_rows, kv_width = wide_ref.shape
    window = k_ref.shape[2]
    heads = sink_ref.shape[1]
    scale = HD ** (-0.5)
    eye = iota((head_rows, heads), 0) == iota((head_rows, heads), 1)
    sink = jnp.sum(jnp.where(eye, sink_ref[...], 0.0), axis=1, keepdims=True)
    own = (iota((head_rows, kv_width), 0) // group_size) == (iota((head_rows, kv_width), 1) // HD)
    slot = iota((1, window), 1)
    for t in range(requests):
        length = len_ref[t]
        newest = length - 1
        behind = lax.rem(newest, window) - slot
        behind = jnp.where(behind < 0, behind + window, behind)
        position = newest - behind
        visible = (position >= 0) & (position >= length - window + 1)
        q = wide_ref[t]
        scores = (
            jnp.dot(q.astype(BF16), k_ref[t], preferred_element_type=F32) * scale
        )
        scores = jnp.where(visible, scores, -1e30)
        fresh = (
            jnp.sum(q * kn_ref[t : t + 1, :].astype(F32), axis=1, keepdims=True) * scale
        )
        highest = jnp.maximum(
            jnp.maximum(jnp.max(scores, axis=1, keepdims=True), fresh), sink
        )
        weights = jnp.exp(scores - highest)
        fresh_weight = jnp.exp(fresh - highest)
        total = jnp.sum(weights, axis=1, keepdims=True) + fresh_weight + jnp.exp(sink - highest)
        probs = (weights / total).astype(BF16)
        fresh_prob = (fresh_weight / total).astype(BF16).astype(F32)
        context = dot_nt(probs, v_ref[t])
        context = context + fresh_prob * vn_ref[t : t + 1, :].astype(F32)
        context = jnp.where(own, context, 0.0)
        folded = jnp.zeros((head_rows, LANES), F32)
        for start in range(0, kv_width, LANES):
            part = context[:, start : min(start + LANES, kv_width)]
            if part.shape[1] < LANES:
                part = jnp.concatenate(
                    [part, jnp.zeros((head_rows, LANES - part.shape[1]), F32)], axis=1
                )
            folded = folded + part
        ctx_ref[t] = folded + pltpu.roll(folded, HD, 1)


def kernel(
    n,
    capacity,
    half,
    q_hbm,
    res_hbm,
    kn_hbm,
    vn_hbm,
    len_hbm,
    sink_hbm,
    gain_hbm,
    ids_hbm,
    logit_hbm,
    k_hbm,
    v_hbm,
    up_hbm,
    down_hbm,
    out_ref,
    q_ref,
    res_ref,
    kn_ref,
    vn_ref,
    len_ref,
    sink_ref,
    gain_ref,
    ids_ref,
    logit_ref,
    k_ref,
    v_ref,
    up_ref,
    down_ref,
    wide_ref,
    ctx_ref,
    hid_ref,
    norm_ref,
    rows_ref,
    ids_wide,
    ids_pad,
    logit_wide,
    logit_pad,
    packed_ref,
    recv_ref,
    act_ref,
    down_half,
    down_peer,
    sent_ref,
    back_ref,
    mix_ref,
    mix_peer,
    load_sem,
    one_send,
    one_recv,
    go_send,
    go_recv,
    fwd_send,
    fwd_recv,
    ret_send,
    ret_recv,
):
    me = lax.axis_index("ep")
    core = lax.axis_index("role")
    group = lax.axis_index("groups")
    peer = (group, me, 1 - core)
    rows, width = res_ref.shape
    heads = width // HD
    experts = n // 2
    group_size = heads // (kn_ref.shape[1] // HD)

    barrier = pltpu.get_barrier_semaphore()
    pl.semaphore_signal(barrier, inc=1, device_id=peer, device_id_type=MESH)

    @pl.loop(1, n)
    def _(step):
        other = lax.rem(me + step, n)
        pl.semaphore_signal(barrier, inc=1, device_id=(group, other, core), device_id_type=MESH)

    loads = [
        pltpu.make_async_copy(src, dst, load_sem.at[i])
        for i, (src, dst) in enumerate(
            (
                (ids_hbm, ids_ref),
                (logit_hbm, logit_ref),
                (q_hbm, q_ref),
                (len_hbm, len_ref),
                (k_hbm, k_ref),
                (kn_hbm, kn_ref),
                (sink_hbm, sink_ref),
                (v_hbm, v_ref),
                (vn_hbm, vn_ref),
                (res_hbm, res_ref),
                (gain_hbm, gain_ref),
                (down_hbm, down_ref),
                (up_hbm, up_ref),
            )
        )
    ]
    for load in loads:
        load.start()
    loads[0].wait()
    loads[1].wait()

    token_rows = 2 * SLOTS
    picks = ids_ref.shape[0]

    def by_token(src, wide, tall, fill):
        wide[...] = jnp.full(wide.shape, fill, wide.dtype)
        wide[:picks, : 2 * rows] = src[...]
        turned = wide[...].T
        tall[...] = jnp.full(tall.shape, fill, tall.dtype)
        for side in range(2):
            tall[side * SLOTS : side * SLOTS + rows, :] = turned[
                side * rows : (side + 1) * rows, :
            ]
        return tall[:, :picks]

    ids = by_token(ids_ref, ids_wide, ids_pad, -1)
    logits = by_token(logit_ref, logit_wide, logit_pad, 0)
    gates = jnp.exp(logits - jnp.max(logits, axis=1, keepdims=True))
    gates = gates / jnp.sum(gates, axis=1, keepdims=True)
    earlier = (iota((token_rows, token_rows), 1) < iota((token_rows, token_rows), 0)).astype(F32)

    def tables(columns, per_expert):
        shape = (token_rows, columns)
        expert = iota(shape, 1) // per_expert
        slot = lax.rem(iota(shape, 1), SLOTS)
        hot = jnp.zeros(shape, F32)
        gate = jnp.zeros(shape, F32)
        for pick in range(ids.shape[1]):
            named = ids[:, pick : pick + 1] == expert
            hot = hot + jnp.where(named, 1.0, 0.0)
            gate = gate + jnp.where(named, gates[:, pick : pick + 1], 0.0)
        place = jnp.dot(earlier.astype(BF16), hot.astype(BF16), preferred_element_type=F32)
        chosen = jnp.where(place == slot.astype(F32), hot, 0.0)
        return chosen, gate * chosen

    send_table, _ = tables(max(experts * SLOTS, LANES), SLOTS)
    send_table = send_table.T[: experts * SLOTS].astype(BF16)
    _, mixing = tables(n * SLOTS, 2 * SLOTS)
    coarse = mixing.astype(BF16)
    fine = (mixing - coarse.astype(F32)).astype(BF16)

    loads[2].wait()
    spread_queries(q_ref, wide_ref, group_size)
    for load in loads[3:11]:
        load.wait()
    attend(wide_ref, kn_ref, vn_ref, k_ref, v_ref, len_ref, sink_ref, ctx_ref, group_size)
    hid_ref[...] = jnp.zeros_like(hid_ref)
    for tile in range((heads + 1) // 2):
        first = ctx_ref[:, 2 * tile, :]
        if 2 * tile + 1 < heads:
            second = ctx_ref[:, 2 * tile + 1, :]
        else:
            second = jnp.zeros_like(first)
        size = min(LANES, width - tile * LANES)
        both = jnp.where(iota(first.shape, 1) < HD, first, second)[:, :size]
        columns = slice(tile * LANES, tile * LANES + size)
        hid_ref[0:rows, columns] = both + res_ref[:, columns].astype(F32)
    hidden = hid_ref[...]
    inverse = lax.rsqrt(jnp.sum(hidden * hidden, axis=1, keepdims=True) / width + 1e-05)
    gain = gain_ref[...].reshape(1, width)
    norm_ref[0] = (hidden[:, :half] * inverse * gain[:, :half]).astype(BF16)
    norm_ref[1] = jnp.zeros(norm_ref.shape[1:], BF16)
    norm_ref[1, :, : width - half] = (
        hidden[:, half:width] * inverse * gain[:, half:]
    ).astype(BF16)

    pl.semaphore_wait(barrier, n)

    def to_peer(src, dst, number):
        return pltpu.make_async_remote_copy(
            src_ref=src,
            dst_ref=dst,
            send_sem=one_send.at[number],
            recv_sem=one_recv.at[number],
            device_id=peer,
            device_id_type=MESH,
        )

    swap_rows = to_peer(norm_ref.at[1 - core], rows_ref.at[core], 0)
    swap_rows.start()
    rows_ref[core] = norm_ref[core]

    swap_rows.wait()
    token_block = rows_ref[...].astype(F32).reshape(token_rows, half).astype(BF16)
    packed = jnp.dot(send_table, token_block, preferred_element_type=F32)
    packed_ref[...] = packed.reshape(experts, SLOTS, half).astype(BF16)

    used = pl.ds(0, capacity)

    def go(step):
        other = lax.rem(me + step, n)
        return pltpu.make_async_remote_copy(
            src_ref=packed_ref.at[other // 2, used],
            dst_ref=recv_ref.at[core, me, used],
            send_sem=go_send.at[other],
            recv_sem=go_recv.at[me],
            device_id=(group, other, core),
            device_id_type=MESH,
        )

    def come(step, buffer, send_sem, recv_sem):
        source = lax.rem(me + n - step, n)
        return source, pltpu.make_async_remote_copy(
            src_ref=buffer,
            dst_ref=buffer,
            send_sem=send_sem.at[source],
            recv_sem=recv_sem.at[source],
            device_id=peer,
            device_id_type=MESH,
        )

    def far_first(turn):
        return 1 + lax.rem(turn + n // 2 - 2, n - 1)

    @pl.loop(1, n)
    def _(turn):
        go(far_first(turn)).start()

    loads[11].wait()
    down_half[0] = down_ref[:, :half]
    down_half[1] = jnp.zeros(down_half.shape[1:], BF16)
    down_half[1, :, : width - half] = down_ref[:, half:]
    swap_down = to_peer(down_half.at[1 - core], down_peer, 1)
    swap_down.start()

    def forward(src, source):
        return pltpu.make_async_remote_copy(
            src_ref=src,
            dst_ref=recv_ref.at[core, source, used],
            send_sem=fwd_send.at[source],
            recv_sem=fwd_recv.at[source],
            device_id=peer,
            device_id_type=MESH,
        )

    recv_ref[core, me] = packed_ref[me // 2]
    forward(packed_ref.at[me // 2, used], me).start()

    @pl.loop(1, n)
    def _(turn):
        step = far_first(n - turn)
        source = lax.rem(me + n - step, n)
        block = recv_ref.at[core, source, used]
        come(step, block, go_send, go_recv)[1].wait_recv()
        forward(block, source).start()

    @pl.loop(0, n)
    def _(source):
        block = recv_ref.at[1 - core, source, used]
        pltpu.make_async_remote_copy(
            src_ref=block,
            dst_ref=block,
            send_sem=fwd_send.at[source],
            recv_sem=fwd_recv.at[source],
            device_id=peer,
            device_id_type=MESH,
        ).wait_recv()

    loads[12].wait()
    chunk = min(n, 16)
    chunk_rows = chunk * SLOTS

    @pl.loop(0, n // chunk)
    def _(part):
        blocks = pl.ds(part * chunk, chunk)
        low = recv_ref[0, blocks].astype(F32).reshape(chunk_rows, half).astype(BF16)
        high = recv_ref[1, blocks].astype(F32).reshape(chunk_rows, half).astype(BF16)
        value = dot_nt(low, up_ref[:, :half]) + dot_nt(high[:, : width - half], up_ref[:, half:])
        value = value / (1.0 + jnp.exp(-value))
        act_ref[core, pl.ds(pl.multiple_of(part * chunk_rows, chunk_rows), chunk_rows), :] = (
            value.astype(BF16)
        )

    swap_act = to_peer(act_ref.at[core], act_ref.at[core], 2)
    swap_act.start()
    swap_down.wait()
    swap_act.wait()

    @pl.loop(0, n // chunk)
    def _(part):
        blocks = pl.ds(part * chunk, chunk)
        place = pl.ds(pl.multiple_of(part * chunk_rows, chunk_rows), chunk_rows)
        value = jnp.dot(
            act_ref[core, place, :], down_half[core], preferred_element_type=F32
        ) + jnp.dot(act_ref[1 - core, place, :], down_peer[...], preferred_element_type=F32)
        sent_ref[blocks] = value.reshape(chunk, SLOTS, half).astype(BF16)

    def give_back(step):
        other = lax.rem(me + step, n)
        return pltpu.make_async_remote_copy(
            src_ref=sent_ref.at[other, used],
            dst_ref=back_ref.at[me, used],
            send_sem=ret_send.at[other],
            recv_sem=ret_recv.at[me],
            device_id=(group, other, core),
            device_id_type=MESH,
        )

    @pl.loop(1, n)
    def _(turn):
        give_back(far_first(turn)).start()

    back_ref[me] = sent_ref[me]

    @pl.loop(1, n)
    def _(step):
        go(step).wait_send()

    @pl.loop(0, n)
    def _(source):
        forward(recv_ref.at[core, source, used], source).wait_send()

    @pl.loop(1, n)
    def _(step):
        source = lax.rem(me + n - step, n)
        come(step, back_ref.at[source, used], ret_send, ret_recv)[1].wait_recv()

    returned = back_ref[...].astype(F32)
    returned = jnp.where(iota(returned.shape, 1) < capacity, returned, 0.0)
    returned = returned.reshape(n * SLOTS, half).astype(BF16)
    mixed = jnp.dot(coarse, returned, preferred_element_type=F32) + jnp.dot(
        fine, returned, preferred_element_type=F32
    )
    mix_ref[...] = mixed.reshape(2, SLOTS, half).astype(BF16)
    swap_mix = to_peer(mix_ref.at[1 - core], mix_peer, 3)
    swap_mix.start()
    mine = jnp.where(core == 0, mixed[:SLOTS], mixed[SLOTS:])

    @pl.loop(1, n)
    def _(step):
        give_back(step).wait_send()

    swap_mix.wait()
    theirs = mix_peer[...].astype(F32)
    low = jnp.where(core == 0, mine, theirs)
    high = jnp.where(core == 0, theirs, mine)
    out_ref[:, :half] = (hid_ref[:, :half] + low)[:rows]
    out_ref[:, half:] = (hid_ref[:, half:width] + high[:, : width - half])[:rows]


def local(
    residual,
    queries,
    key_new,
    value_new,
    key_cache,
    value_cache,
    lengths,
    sink_logits,
    norm_gain,
    route_ids,
    route_logits,
    up_weight,
    down_weight,
):
    n = lax.axis_size("ep")
    experts = n // 2
    pair_count, pick_count = route_ids.shape
    capacity = min(pair_count, max(2, (pair_count * pick_count + experts - 1) // experts))
    rows, width = residual.shape
    half = -(-width // (4 * LANES)) * 2 * LANES
    heads = width // HD
    head_rows = -(-heads // 8) * 8
    depth = up_weight.shape[1]
    vmem = pl.BlockSpec(memory_space=pltpu.VMEM)
    anywhere = pl.BlockSpec(memory_space=pl.ANY)
    dma = pltpu.SemaphoreType.DMA
    return pl.pallas_call(
        functools.partial(kernel, n, capacity, half),
        out_shape=jax.ShapeDtypeStruct((rows, width), F32),
        in_specs=[anywhere] * 13,
        out_specs=vmem,
        scratch_shapes=[
            pltpu.VMEM(queries.shape, BF16),
            pltpu.VMEM(residual.shape, BF16),
            pltpu.VMEM(key_new.shape, BF16),
            pltpu.VMEM(value_new.shape, BF16),
            pltpu.SMEM(lengths.shape, jnp.int32),
            pltpu.VMEM((1, heads), F32),
            pltpu.VMEM(norm_gain.shape, F32),
            pltpu.VMEM(route_ids.shape[::-1], jnp.int32),
            pltpu.VMEM(route_ids.shape[::-1], F32),
            pltpu.VMEM((rows, key_cache.shape[2], key_cache.shape[1]), BF16),
            pltpu.VMEM((rows, key_cache.shape[2], key_cache.shape[1]), BF16),
            pltpu.VMEM((depth, width), BF16),
            pltpu.VMEM(down_weight.shape, BF16),
            pltpu.VMEM((rows, head_rows, key_new.shape[1]), F32),
            pltpu.VMEM((rows, head_rows, LANES), F32),
            pltpu.VMEM((SLOTS, 2 * half), F32),
            pltpu.VMEM((2, SLOTS, half), BF16),
            pltpu.VMEM((2, SLOTS, half), BF16),
            pltpu.VMEM((8, LANES), jnp.int32),
            pltpu.VMEM((2 * SLOTS, 8), jnp.int32),
            pltpu.VMEM((8, LANES), F32),
            pltpu.VMEM((2 * SLOTS, 8), F32),
            pltpu.VMEM((experts, SLOTS, half), BF16),
            pltpu.VMEM((2, n, SLOTS, half), BF16),
            pltpu.VMEM((2, n * SLOTS, depth), BF16),
            pltpu.VMEM((2, depth, half), BF16),
            pltpu.VMEM((depth, half), BF16),
            pltpu.VMEM((n, SLOTS, half), BF16),
            pltpu.VMEM((n, SLOTS, half), BF16),
            pltpu.VMEM((2, SLOTS, half), BF16),
            pltpu.VMEM((SLOTS, half), BF16),
            dma((13,)),
            dma((4,)),
            dma((4,)),
            dma((n,)),
            dma((n,)),
            dma((n,)),
            dma((n,)),
            dma((n,)),
            dma((n,)),
        ],
        compiler_params=pltpu.CompilerParams(
            collective_id=0, has_side_effects=True, vmem_limit_bytes=60 * 1024 * 1024
        ),
    )(
        queries,
        residual,
        key_new,
        value_new,
        lengths,
        sink_logits.reshape(1, -1),
        norm_gain,
        route_ids.T,
        route_logits.T,
        jnp.swapaxes(key_cache, 1, 2),
        jnp.swapaxes(value_cache, 1, 2),
        up_weight.T,
        down_weight,
    ).astype(BF16)


def solution(mesh):
    placed = (
        P(("groups", "ep", "role"), None),
        P(("groups", "ep", "role"), None),
        P(("groups", "ep", "role"), None),
        P(("groups", "ep", "role"), None),
        P(("groups", "ep", "role"), None, None),
        P(("groups", "ep", "role"), None, None),
        P(("groups", "ep", "role")),
        P(),
        P(),
        P(("groups", "ep"), None),
        P(("groups", "ep"), None),
        P(None, ("ep", "role")),
        P(("ep", "role"), None),
    )
    return jax.shard_map(
        local,
        mesh=mesh,
        in_specs=placed,
        out_specs=P(("groups", "ep", "role"), None),
        check_vma=False,
    )
```

```python
import functools

import jax
import jax.numpy as jnp
from jax import lax
from jax.experimental import pallas as pl
from jax.experimental.pallas import tpu as pltpu
from jax.sharding import PartitionSpec as P

HD = 64
LANES = 128
SLOTS = 8
MESH = pl.DeviceIdType.MESH
BF16 = jnp.bfloat16
F32 = jnp.float32


def iota(shape, dim):
    return lax.broadcasted_iota(jnp.int32, shape, dim)


def dot_nt(a, b):
    return lax.dot_general(a, b, (((1,), (1,)), ((), ())), preferred_element_type=F32)


def spread_queries(q_ref, wide_ref, group_size):
    rows, width = q_ref.shape
    heads = width // HD
    wide_ref[...] = jnp.zeros_like(wide_ref)
    kv_width = wide_ref.shape[2]
    for head in range(heads):
        tile, half = head // 2, head % 2
        size = min(LANES, width - tile * LANES)
        block = q_ref[:, tile * LANES : tile * LANES + size].astype(F32)
        if size < LANES:
            block = jnp.concatenate([block, jnp.zeros((rows, LANES - size), F32)], axis=1)
        kv = head // group_size
        if half != kv % 2:
            block = pltpu.roll(block, HD, 1)
        lane = iota(block.shape, 1)
        block = jnp.where((lane // HD) == (kv % 2), block, 0.0)
        start = (kv // 2) * LANES
        stop = min(start + LANES, kv_width)
        wide_ref[:, head, start:stop] = block[:, : stop - start]


def attend(wide_ref, kn_ref, vn_ref, k_ref, v_ref, len_ref, sink_ref, ctx_ref, group_size):
    requests, head_rows, kv_width = wide_ref.shape
    window = k_ref.shape[2]
    heads = sink_ref.shape[1]
    scale = HD ** (-0.5)
    eye = iota((head_rows, heads), 0) == iota((head_rows, heads), 1)
    sink = jnp.sum(jnp.where(eye, sink_ref[...], 0.0), axis=1, keepdims=True)
    own = (iota((head_rows, kv_width), 0) // group_size) == (iota((head_rows, kv_width), 1) // HD)
    slot = iota((1, window), 1)
    for t in range(requests):
        length = len_ref[t]
        newest = length - 1
        behind = lax.rem(newest, window) - slot
        behind = jnp.where(behind < 0, behind + window, behind)
        position = newest - behind
        visible = (position >= 0) & (position >= length - window + 1)
        q = wide_ref[t]
        scores = (
            jnp.dot(q.astype(BF16), k_ref[t], preferred_element_type=F32) * scale
        )
        scores = jnp.where(visible, scores, -1e30)
        fresh = (
            jnp.sum(q * kn_ref[t : t + 1, :].astype(F32), axis=1, keepdims=True) * scale
        )
        highest = jnp.maximum(
            jnp.maximum(jnp.max(scores, axis=1, keepdims=True), fresh), sink
        )
        weights = jnp.exp(scores - highest)
        fresh_weight = jnp.exp(fresh - highest)
        total = jnp.sum(weights, axis=1, keepdims=True) + fresh_weight + jnp.exp(sink - highest)
        probs = (weights / total).astype(BF16)
        fresh_prob = (fresh_weight / total).astype(BF16).astype(F32)
        context = dot_nt(probs, v_ref[t])
        context = context + fresh_prob * vn_ref[t : t + 1, :].astype(F32)
        context = jnp.where(own, context, 0.0)
        folded = jnp.zeros((head_rows, LANES), F32)
        for start in range(0, kv_width, LANES):
            part = context[:, start : min(start + LANES, kv_width)]
            if part.shape[1] < LANES:
                part = jnp.concatenate(
                    [part, jnp.zeros((head_rows, LANES - part.shape[1]), F32)], axis=1
                )
            folded = folded + part
        ctx_ref[t] = folded + pltpu.roll(folded, HD, 1)


def kernel(
    n,
    capacity,
    half,
    q_hbm,
    res_hbm,
    kn_hbm,
    vn_hbm,
    len_hbm,
    sink_hbm,
    gain_hbm,
    ids_hbm,
    logit_hbm,
    k_hbm,
    v_hbm,
    up_hbm,
    down_hbm,
    out_ref,
    q_ref,
    res_ref,
    kn_ref,
    vn_ref,
    len_ref,
    sink_ref,
    gain_ref,
    ids_ref,
    logit_ref,
    k_ref,
    v_ref,
    up_ref,
    down_ref,
    wide_ref,
    ctx_ref,
    hid_ref,
    norm_ref,
    rows_ref,
    ids_wide,
    ids_pad,
    logit_wide,
    logit_pad,
    packed_ref,
    recv_ref,
    act_ref,
    down_half,
    down_peer,
    sent_ref,
    back_ref,
    mix_ref,
    mix_peer,
    load_sem,
    one_send,
    one_recv,
    go_send,
    go_recv,
    fwd_send,
    fwd_recv,
    ret_send,
    ret_recv,
):
    me = lax.axis_index("ep")
    core = lax.axis_index("role")
    group = lax.axis_index("groups")
    peer = (group, me, 1 - core)
    rows, width = res_ref.shape
    heads = width // HD
    experts = n // 2
    group_size = heads // (kn_ref.shape[1] // HD)

    barrier = pltpu.get_barrier_semaphore()
    pl.semaphore_signal(barrier, inc=1, device_id=peer, device_id_type=MESH)

    @pl.loop(1, n)
    def _(step):
        other = lax.rem(me + step, n)
        pl.semaphore_signal(barrier, inc=1, device_id=(group, other, core), device_id_type=MESH)

    loads = [
        pltpu.make_async_copy(src, dst, load_sem.at[i])
        for i, (src, dst) in enumerate(
            (
                (ids_hbm, ids_ref),
                (logit_hbm, logit_ref),
                (q_hbm, q_ref),
                (len_hbm, len_ref),
                (k_hbm, k_ref),
                (kn_hbm, kn_ref),
                (sink_hbm, sink_ref),
                (v_hbm, v_ref),
                (vn_hbm, vn_ref),
                (res_hbm, res_ref),
                (gain_hbm, gain_ref),
                (down_hbm, down_ref),
                (up_hbm, up_ref),
            )
        )
    ]
    for load in loads:
        load.start()
    loads[0].wait()
    loads[1].wait()

    token_rows = 2 * SLOTS
    picks = ids_ref.shape[0]

    def by_token(src, wide, tall, fill):
        wide[...] = jnp.full(wide.shape, fill, wide.dtype)
        wide[:picks, : 2 * rows] = src[...]
        turned = wide[...].T
        tall[...] = jnp.full(tall.shape, fill, tall.dtype)
        for side in range(2):
            tall[side * SLOTS : side * SLOTS + rows, :] = turned[
                side * rows : (side + 1) * rows, :
            ]
        return tall[:, :picks]

    ids = by_token(ids_ref, ids_wide, ids_pad, -1)
    logits = by_token(logit_ref, logit_wide, logit_pad, 0)
    gates = jnp.exp(logits - jnp.max(logits, axis=1, keepdims=True))
    gates = gates / jnp.sum(gates, axis=1, keepdims=True)
    earlier = (iota((token_rows, token_rows), 1) < iota((token_rows, token_rows), 0)).astype(F32)

    def tables(columns, per_expert):
        shape = (token_rows, columns)
        expert = iota(shape, 1) // per_expert
        slot = lax.rem(iota(shape, 1), SLOTS)
        hot = jnp.zeros(shape, F32)
        gate = jnp.zeros(shape, F32)
        for pick in range(ids.shape[1]):
            named = ids[:, pick : pick + 1] == expert
            hot = hot + jnp.where(named, 1.0, 0.0)
            gate = gate + jnp.where(named, gates[:, pick : pick + 1], 0.0)
        place = jnp.dot(earlier.astype(BF16), hot.astype(BF16), preferred_element_type=F32)
        chosen = jnp.where(place == slot.astype(F32), hot, 0.0)
        return chosen, gate * chosen

    send_table, _ = tables(max(experts * SLOTS, LANES), SLOTS)
    send_table = send_table.T[: experts * SLOTS].astype(BF16)
    _, mixing = tables(n * SLOTS, 2 * SLOTS)
    coarse = mixing.astype(BF16)
    fine = (mixing - coarse.astype(F32)).astype(BF16)

    loads[2].wait()
    spread_queries(q_ref, wide_ref, group_size)
    for load in loads[3:11]:
        load.wait()
    attend(wide_ref, kn_ref, vn_ref, k_ref, v_ref, len_ref, sink_ref, ctx_ref, group_size)
    hid_ref[...] = jnp.zeros_like(hid_ref)
    for tile in range((heads + 1) // 2):
        first = ctx_ref[:, 2 * tile, :]
        if 2 * tile + 1 < heads:
            second = ctx_ref[:, 2 * tile + 1, :]
        else:
            second = jnp.zeros_like(first)
        size = min(LANES, width - tile * LANES)
        both = jnp.where(iota(first.shape, 1) < HD, first, second)[:, :size]
        columns = slice(tile * LANES, tile * LANES + size)
        hid_ref[0:rows, columns] = both + res_ref[:, columns].astype(F32)
    hidden = hid_ref[...]
    inverse = lax.rsqrt(jnp.sum(hidden * hidden, axis=1, keepdims=True) / width + 1e-05)
    gain = gain_ref[...].reshape(1, width)
    norm_ref[0] = (hidden[:, :half] * inverse * gain[:, :half]).astype(BF16)
    norm_ref[1] = jnp.zeros(norm_ref.shape[1:], BF16)
    norm_ref[1, :, : width - half] = (
        hidden[:, half:width] * inverse * gain[:, half:]
    ).astype(BF16)

    pl.semaphore_wait(barrier, n)

    def to_peer(src, dst, number):
        return pltpu.make_async_remote_copy(
            src_ref=src,
            dst_ref=dst,
            send_sem=one_send.at[number],
            recv_sem=one_recv.at[number],
            device_id=peer,
            device_id_type=MESH,
        )

    swap_rows = to_peer(norm_ref.at[1 - core], rows_ref.at[core], 0)
    swap_rows.start()
    rows_ref[core] = norm_ref[core]

    swap_rows.wait()
    token_block = rows_ref[...].astype(F32).reshape(token_rows, half).astype(BF16)
    packed = jnp.dot(send_table, token_block, preferred_element_type=F32)
    packed_ref[...] = packed.reshape(experts, SLOTS, half).astype(BF16)

    used = pl.ds(0, capacity)

    def go(step):
        other = lax.rem(me + step, n)
        return pltpu.make_async_remote_copy(
            src_ref=packed_ref.at[other // 2, used],
            dst_ref=recv_ref.at[core, me, used],
            send_sem=go_send.at[other],
            recv_sem=go_recv.at[me],
            device_id=(group, other, core),
            device_id_type=MESH,
        )

    def come(step, buffer, send_sem, recv_sem):
        source = lax.rem(me + n - step, n)
        return source, pltpu.make_async_remote_copy(
            src_ref=buffer,
            dst_ref=buffer,
            send_sem=send_sem.at[source],
            recv_sem=recv_sem.at[source],
            device_id=peer,
            device_id_type=MESH,
        )

    @pl.loop(1, n)
    def _(step):
        go(step).start()

    loads[11].wait()
    down_half[0] = down_ref[:, :half]
    down_half[1] = jnp.zeros(down_half.shape[1:], BF16)
    down_half[1, :, : width - half] = down_ref[:, half:]
    swap_down = to_peer(down_half.at[1 - core], down_peer, 1)
    swap_down.start()

    def forward(src, source):
        return pltpu.make_async_remote_copy(
            src_ref=src,
            dst_ref=recv_ref.at[core, source, used],
            send_sem=fwd_send.at[source],
            recv_sem=fwd_recv.at[source],
            device_id=peer,
            device_id_type=MESH,
        )

    recv_ref[core, me] = packed_ref[me // 2]
    forward(packed_ref.at[me // 2, used], me).start()

    @pl.loop(1, n)
    def _(step):
        source = lax.rem(me + n - step, n)
        block = recv_ref.at[core, source, used]
        come(step, block, go_send, go_recv)[1].wait_recv()
        forward(block, source).start()

    @pl.loop(0, n)
    def _(source):
        block = recv_ref.at[1 - core, source, used]
        pltpu.make_async_remote_copy(
            src_ref=block,
            dst_ref=block,
            send_sem=fwd_send.at[source],
            recv_sem=fwd_recv.at[source],
            device_id=peer,
            device_id_type=MESH,
        ).wait_recv()

    loads[12].wait()
    chunk = min(n, 16)
    chunk_rows = chunk * SLOTS

    @pl.loop(0, n // chunk)
    def _(part):
        blocks = pl.ds(part * chunk, chunk)
        low = recv_ref[0, blocks].astype(F32).reshape(chunk_rows, half).astype(BF16)
        high = recv_ref[1, blocks].astype(F32).reshape(chunk_rows, half).astype(BF16)
        value = dot_nt(low, up_ref[:, :half]) + dot_nt(high[:, : width - half], up_ref[:, half:])
        value = value / (1.0 + jnp.exp(-value))
        act_ref[core, pl.ds(pl.multiple_of(part * chunk_rows, chunk_rows), chunk_rows), :] = (
            value.astype(BF16)
        )

    swap_act = to_peer(act_ref.at[core], act_ref.at[core], 2)
    swap_act.start()
    swap_down.wait()
    swap_act.wait()

    @pl.loop(0, n // chunk)
    def _(part):
        blocks = pl.ds(part * chunk, chunk)
        place = pl.ds(pl.multiple_of(part * chunk_rows, chunk_rows), chunk_rows)
        value = jnp.dot(
            act_ref[core, place, :], down_half[core], preferred_element_type=F32
        ) + jnp.dot(act_ref[1 - core, place, :], down_peer[...], preferred_element_type=F32)
        sent_ref[blocks] = value.reshape(chunk, SLOTS, half).astype(BF16)

    def give_back(step):
        other = lax.rem(me + step, n)
        return pltpu.make_async_remote_copy(
            src_ref=sent_ref.at[other, used],
            dst_ref=back_ref.at[me, used],
            send_sem=ret_send.at[other],
            recv_sem=ret_recv.at[me],
            device_id=(group, other, core),
            device_id_type=MESH,
        )

    @pl.loop(1, n)
    def _(step):
        give_back(step).start()

    back_ref[me] = sent_ref[me]

    @pl.loop(1, n)
    def _(step):
        go(step).wait_send()

    @pl.loop(0, n)
    def _(source):
        forward(recv_ref.at[core, source, used], source).wait_send()

    @pl.loop(1, n)
    def _(step):
        source = lax.rem(me + n - step, n)
        come(step, back_ref.at[source, used], ret_send, ret_recv)[1].wait_recv()

    returned = back_ref[...].astype(F32)
    returned = jnp.where(iota(returned.shape, 1) < capacity, returned, 0.0)
    returned = returned.reshape(n * SLOTS, half).astype(BF16)
    mixed = jnp.dot(coarse, returned, preferred_element_type=F32) + jnp.dot(
        fine, returned, preferred_element_type=F32
    )
    mix_ref[...] = mixed.reshape(2, SLOTS, half).astype(BF16)
    swap_mix = to_peer(mix_ref.at[1 - core], mix_peer, 3)
    swap_mix.start()
    mine = jnp.where(core == 0, mixed[:SLOTS], mixed[SLOTS:])

    @pl.loop(1, n)
    def _(step):
        give_back(step).wait_send()

    swap_mix.wait()
    theirs = mix_peer[...].astype(F32)
    low = jnp.where(core == 0, mine, theirs)
    high = jnp.where(core == 0, theirs, mine)
    out_ref[:, :half] = (hid_ref[:, :half] + low)[:rows]
    out_ref[:, half:] = (hid_ref[:, half:width] + high[:, : width - half])[:rows]


def local(
    residual,
    queries,
    key_new,
    value_new,
    key_cache,
    value_cache,
    lengths,
    sink_logits,
    norm_gain,
    route_ids,
    route_logits,
    up_weight,
    down_weight,
):
    n = lax.axis_size("ep")
    experts = n // 2
    pair_count, pick_count = route_ids.shape
    capacity = min(pair_count, max(2, (pair_count * pick_count + experts - 1) // experts))
    rows, width = residual.shape
    half = -(-width // (4 * LANES)) * 2 * LANES
    heads = width // HD
    head_rows = -(-heads // 8) * 8
    depth = up_weight.shape[1]
    vmem = pl.BlockSpec(memory_space=pltpu.VMEM)
    anywhere = pl.BlockSpec(memory_space=pl.ANY)
    dma = pltpu.SemaphoreType.DMA
    return pl.pallas_call(
        functools.partial(kernel, n, capacity, half),
        out_shape=jax.ShapeDtypeStruct((rows, width), F32),
        in_specs=[anywhere] * 13,
        out_specs=vmem,
        scratch_shapes=[
            pltpu.VMEM(queries.shape, BF16),
            pltpu.VMEM(residual.shape, BF16),
            pltpu.VMEM(key_new.shape, BF16),
            pltpu.VMEM(value_new.shape, BF16),
            pltpu.SMEM(lengths.shape, jnp.int32),
            pltpu.VMEM((1, heads), F32),
            pltpu.VMEM(norm_gain.shape, F32),
            pltpu.VMEM(route_ids.shape[::-1], jnp.int32),
            pltpu.VMEM(route_ids.shape[::-1], F32),
            pltpu.VMEM((rows, key_cache.shape[2], key_cache.shape[1]), BF16),
            pltpu.VMEM((rows, key_cache.shape[2], key_cache.shape[1]), BF16),
            pltpu.VMEM((depth, width), BF16),
            pltpu.VMEM(down_weight.shape, BF16),
            pltpu.VMEM((rows, head_rows, key_new.shape[1]), F32),
            pltpu.VMEM((rows, head_rows, LANES), F32),
            pltpu.VMEM((SLOTS, 2 * half), F32),
            pltpu.VMEM((2, SLOTS, half), BF16),
            pltpu.VMEM((2, SLOTS, half), BF16),
            pltpu.VMEM((8, LANES), jnp.int32),
            pltpu.VMEM((2 * SLOTS, 8), jnp.int32),
            pltpu.VMEM((8, LANES), F32),
            pltpu.VMEM((2 * SLOTS, 8), F32),
            pltpu.VMEM((experts, SLOTS, half), BF16),
            pltpu.VMEM((2, n, SLOTS, half), BF16),
            pltpu.VMEM((2, n * SLOTS, depth), BF16),
            pltpu.VMEM((2, depth, half), BF16),
            pltpu.VMEM((depth, half), BF16),
            pltpu.VMEM((n, SLOTS, half), BF16),
            pltpu.VMEM((n, SLOTS, half), BF16),
            pltpu.VMEM((2, SLOTS, half), BF16),
            pltpu.VMEM((SLOTS, half), BF16),
            dma((13,)),
            dma((4,)),
            dma((4,)),
            dma((n,)),
            dma((n,)),
            dma((n,)),
            dma((n,)),
            dma((n,)),
            dma((n,)),
        ],
        compiler_params=pltpu.CompilerParams(
            collective_id=0, has_side_effects=True, vmem_limit_bytes=60 * 1024 * 1024
        ),
    )(
        queries,
        residual,
        key_new,
        value_new,
        lengths,
        sink_logits.reshape(1, -1),
        norm_gain,
        route_ids.T,
        route_logits.T,
        jnp.swapaxes(key_cache, 1, 2),
        jnp.swapaxes(value_cache, 1, 2),
        up_weight.T,
        down_weight,
    ).astype(BF16)


def solution(mesh):
    placed = (
        P(("groups", "ep", "role"), None),
        P(("groups", "ep", "role"), None),
        P(("groups", "ep", "role"), None),
        P(("groups", "ep", "role"), None),
        P(("groups", "ep", "role"), None, None),
        P(("groups", "ep", "role"), None, None),
        P(("groups", "ep", "role")),
        P(),
        P(),
        P(("groups", "ep"), None),
        P(("groups", "ep"), None),
        P(None, ("ep", "role")),
        P(("ep", "role"), None),
    )
    return jax.shard_map(
        local,
        mesh=mesh,
        in_specs=placed,
        out_specs=P(("groups", "ep", "role"), None),
        check_vma=False,
    )
```
